32 devices in a mesh: blk: 4 (over y, x), grp: 8 (over z, core).
Axes of the slice: x: 2, y: 2, z: 4, core: 2. Of those that a mesh axis runs over, the one named last changes fastest.
Arguments:
- points: float32 [3, 4096], P(None, ('blk', 'grp')), may hold values from 0 to 1
- labels: int32 [4096], P(('blk', 'grp')), may hold values 0 or 1
- shape_scale: float32 [4096], P(('blk', 'grp')), may hold values from 0.1 to 0.4
- krylov_basis: float32 [8, 32, 4096], P(None, None, ('blk', 'grp')), may hold values from -6 to 6
- sketch: float32 [1024, 4096], P(None, ('blk', 'grp')), may hold values from -0.09375 to 0.09375
- sketched_basis: float32 [8, 32, 1024], replicated, may hold values from -0.1875 to 0.1875
Outputs:
- next_vector: float32 [32, 4096], P(None, ('blk', 'grp'))
- coefficients: float32 [8, 32], replicated
- sketch_next: float32 [32, 1024], replicated
- norms: float32 [32], replicated
The draws below stay inside these ranges and needn't reach their ends.
All inputs are finite; a program needn't handle non-finite values. No bound on the sum of `labels` on one device may be relied on, other than what follows from the above.
Results may differ from the reference program's by a relative error of at most 0.0003.
Values sent between devices are 32-bit elements; how exact they have to be, the bound alone decides.
A program may use at most 64 MiB of HBM per device.

```python
import math
import jax
import jax.numpy as jnp
from jax import lax

SYSTEMS = 32
KRYLOV = 8
SKETCH = 1024
N = 4096


def draw_points(key, part):
    first_key = jax.random.fold_in(key, 11)
    second_key = jax.random.fold_in(key, 12)
    third_key = jax.random.fold_in(key, 13)
    across = jax.random.uniform(first_key, (N,), jnp.float32)
    depth = jax.random.uniform(second_key, (N,), jnp.float32)
    jitter = jax.random.uniform(third_key, (N,), jnp.float32)
    ordering = jnp.arange(N).astype(jnp.float32)
    height = (ordering + jitter) / N
    return jnp.stack([across, depth, height], axis=0).astype(jnp.float32)


def place_ends(drawn, key, smallest, top_value):
    place = [jax.random.randint(jax.random.fold_in(key, axis), (), 0, length) for axis, length in enumerate(drawn.shape)]
    widest = drawn.shape.index(max(drawn.shape))
    neighbour = place[:widest] + [(place[widest] + 1) % drawn.shape[widest]] + place[widest + 1:]
    return drawn.at[tuple(place)].set(smallest).at[tuple(neighbour)].set(top_value)


def block_levels(rng, dims, split, smallest, largest):
    def one(position, shards_of):
        draws = jax.random.uniform(jax.random.fold_in(jax.random.fold_in(rng, 6), position), (shards_of,), jnp.float32, smallest / len(split), largest / len(split))
        return jnp.repeat(jnp.exp(draws), dims[position] // shards_of).reshape((-1,) + (1,) * (len(dims) - position - 1))

    factor_of = one(*split[0])
    for cut in split[1:]:
        factor_of = factor_of * one(*cut)
    return factor_of


def gaussian(key, shape, width, bound, cuts=(), held_as=jnp.bfloat16):
    values = width * jax.random.normal(key, shape, jnp.float32)
    if cuts:
        values = values * block_levels(key, shape, cuts, -0.22, 0.18)
    return jnp.clip(values, -bound, bound).astype(held_as)


def setup_inputs(seed: int = 0) -> dict:
    key_list = jax.random.split(jax.random.key(seed), 7)
    points = draw_points(jax.random.fold_in(key_list[6], 71), 0)
    labels = place_ends((jax.random.randint(key_list[1], (N,), 0, 4) < 3).astype(jnp.int32), jax.random.fold_in(key_list[1], 1), 0, 1)
    shape_scale = jnp.clip(jnp.exp(math.log(0.4) - 1.3862944 * jax.random.uniform(key_list[2], (N,), jnp.float32) ** block_levels(key_list[2], (N,), ((0, 32),), -0.2, 0.2)), 0.1, 0.4)
    krylov_basis = gaussian(key_list[3], (KRYLOV, SYSTEMS, N), 1.0, 6.0, ((2, 32),), jnp.float32)
    sketch = gaussian(key_list[4], (SKETCH, N), N ** -0.5, 0.09375, ((1, 32),), jnp.float32)
    sketched_basis = gaussian(key_list[5], (KRYLOV, SYSTEMS, SKETCH), SKETCH ** -0.5, 0.1875, (), jnp.float32)
    return dict(points=points, labels=labels, shape_scale=shape_scale, krylov_basis=krylov_basis, sketch=sketch, sketched_basis=sketched_basis)


def kernel_terms(target_points, target_labels, source_block):
    source_points = source_block[0:3]
    scales = source_block[3]
    weights_block = source_block[4:]
    delta_x = source_points[0][:, None] - target_points[0][None, :]
    delta_y = source_points[1][:, None] - target_points[1][None, :]
    delta_z = source_points[2][:, None] - target_points[2][None, :]
    radius_sq = delta_x * delta_x + delta_y * delta_y + delta_z * delta_z
    squared_scale = (scales * scales)[:, None]
    shifted = radius_sq + squared_scale
    inverse = lax.rsqrt(shifted)
    boundary = shifted * inverse
    interior = (3.0 * squared_scale + 2.0 * radius_sq) * inverse * inverse * inverse
    kernel = jnp.where(target_labels[None, :] == 1, interior, boundary)
    return jnp.dot(weights_block, kernel, precision=lax.Precision.HIGHEST, preferred_element_type=jnp.float32)

def block_size(length, wanted):
    return wanted if length % wanted == 0 else length

def reference(points, labels, shape_scale, krylov_basis, sketch, sketched_basis):
    sources = jnp.concatenate([points, shape_scale[None, :], krylov_basis[KRYLOV - 1]], axis=0)
    width_rows = sources.shape[0]
    tblock = block_size(N, 2048)
    sblock = block_size(N, 2048)
    source_blocks = jnp.transpose(sources.reshape(width_rows, N // sblock, sblock), (1, 0, 2))
    target_blocks = jnp.transpose(points.reshape(3, N // tblock, tblock), (1, 0, 2))
    label_blocks = labels.reshape(N // tblock, tblock)

    def one_target(packed):
        target_points, target_labels = packed

        def over_sources(running, block):
            return (running + kernel_terms(target_points, target_labels, block), None)
        start_value = jnp.zeros((SYSTEMS, tblock), jnp.float32)
        result, unused = lax.scan(over_sources, start_value, source_blocks)
        return result
    pieces = lax.map(one_target, (target_blocks, label_blocks))
    image = jnp.transpose(pieces, (1, 0, 2)).reshape(SYSTEMS, N) / jnp.sqrt(jnp.float32(N))
    sketched = lax.dot_general(image, sketch, (((1,), (1,)), ((), ())), precision=lax.Precision.HIGHEST, preferred_element_type=jnp.float32)
    coefficients = jnp.einsum('jrk,rk->jr', sketched_basis, sketched, precision=lax.Precision.HIGHEST)
    remainder = sketched - jnp.einsum('jr,jrk->rk', coefficients, sketched_basis, precision=lax.Precision.HIGHEST)
    norms = jnp.sqrt(lax.optimization_barrier(jnp.mean(remainder * remainder, axis=1)) + 1e-06)
    sketch_next = remainder / norms[:, None]
    reduced = image - jnp.einsum('jr,jrn->rn', coefficients, krylov_basis, precision=lax.Precision.HIGHEST)
    next_vector = reduced / norms[:, None]
    return (next_vector, coefficients, sketch_next, norms)
```

```python
import functools
import math

import jax
import jax.numpy as jnp
from jax import lax
from jax.experimental import pallas as pl
from jax.experimental.pallas import tpu as pltpu
from jax.sharding import PartitionSpec as P

MESH = pl.DeviceIdType.MESH
F32 = jnp.float32
BF16 = jnp.bfloat16
NT = (((1,), (1,)), ((), ()))


def split(value):
    high = value.astype(BF16)
    low = (value - high.astype(F32)).astype(BF16)
    return high, low


def nt_dot(left, right):
    return lax.dot_general(left, right, NT, preferred_element_type=F32)


def step_kernel(
    nb, ng,
    points_hbm, labels_hbm, scale_hbm, krylov_hbm, sketch_hbm, basis_hbm,
    next_ref, coef_ref, sketch_next_ref, norms_ref,
    pts, lab, scl, krylov, sketch, basis,
    geo, src_geo, tgt_geo, weights,
    tgx, tgy, tgz, tgl, k_high, k_low, w_cat, acc,
    part, part_in, image_ref, sk_high, sk_low,
    sk_part, sk_in, sk_full, cmat,
    local_sem, geo_send, geo_recv, w_send, w_recv, tgt_send, tgt_recv,
    img_send, img_recv, rs_send, rs_recv, ag_send, ag_recv,
):
    b = lax.axis_index("blk")
    g = lax.axis_index("grp")
    ndev = nb * ng
    me = b * ng + g
    own = pts.shape[1]
    vectors, systems, _ = krylov.shape
    tiles = sk_part.shape[0]
    row_groups = systems // 8
    col_blocks = tiles // row_groups

    def at(d):
        return (d // ng, lax.rem(d, ng))

    def remote(src, dst, send, recv, where):
        return pltpu.make_async_remote_copy(
            src_ref=src, dst_ref=dst, send_sem=send, recv_sem=recv,
            device_id=where, device_id_type=MESH,
        )

    copies = [
        pltpu.make_async_copy(points_hbm, pts, local_sem.at[0]),
        pltpu.make_async_copy(labels_hbm, lab, local_sem.at[1]),
        pltpu.make_async_copy(scale_hbm, scl, local_sem.at[2]),
        pltpu.make_async_copy(krylov_hbm.at[vectors - 1], weights.at[g], local_sem.at[3]),
        pltpu.make_async_copy(sketch_hbm, sketch, local_sem.at[4]),
        pltpu.make_async_copy(krylov_hbm, krylov, local_sem.at[5]),
        pltpu.make_async_copy(basis_hbm, basis, local_sem.at[6]),
    ]
    for copy in copies:
        copy.start()

    barrier = pltpu.get_barrier_semaphore()

    def greet(i, carry):
        pl.semaphore_signal(
            barrier, inc=1, device_id=at(lax.rem(me + i, ndev)), device_id_type=MESH
        )
        return carry

    lax.fori_loop(1, ndev, greet, 0)

    for copy in copies[:3]:
        copy.wait()
    scale = scl[...]
    mine = jnp.concatenate(
        [pts[...], scale * scale, lab[...].astype(F32), jnp.zeros((3, own), F32)], axis=0
    )
    geo[...] = mine
    src_geo[g] = mine
    tgt_geo[b] = mine
    copies[3].wait()
    pl.semaphore_wait(barrier, ndev - 1)

    def geo_copy(peer, slot):
        return remote(geo, src_geo.at[slot], geo_send.at[peer], geo_recv.at[slot], (b, peer))

    def tgt_copy(peer, slot):
        return remote(geo, tgt_geo.at[slot], tgt_send.at[peer], tgt_recv.at[slot], (peer, g))

    def w_copy(peer, slot):
        return remote(
            weights.at[g], weights.at[slot], w_send.at[peer], w_recv.at[slot], (b, peer)
        )

    def over(count, first, self_index, action):
        def step(i, carry):
            action(lax.rem(self_index + i, count))
            return carry

        lax.fori_loop(first, count, step, 0)

    over(nb, 1, b, lambda p: tgt_copy(p, b).start())
    over(ng, 1, g, lambda p: geo_copy(p, g).start())
    over(ng, 1, g, lambda p: w_copy(p, g).start())

    copies[4].wait()
    high, low = split(sketch[...])
    sk_high[...] = high
    sk_low[...] = low

    over(nb, 1, b, lambda p: tgt_copy(p, p).wait_recv())
    for k in range(nb):
        turned = jnp.transpose(tgt_geo[k])
        rows = pl.ds(k * own, own)
        tgx[rows, :] = jnp.broadcast_to(turned[:, 0:1], (own, own))
        tgy[rows, :] = jnp.broadcast_to(turned[:, 1:2], (own, own))
        tgz[rows, :] = jnp.broadcast_to(turned[:, 2:3], (own, own))
        tgl[rows, :] = jnp.broadcast_to(turned[:, 4:5], (own, own))

    def columns(p):
        return pl.ds(pl.multiple_of(p * own, own), own)

    def kernel_block(i, carry):
        p = lax.rem(g + i, ng)

        @pl.when(i > 0)
        def _():
            geo_copy(p, p).wait_recv()

        block = src_geo[p]
        sx, sy, sz, ss = block[0:1], block[1:2], block[2:3], block[3:4]
        for first in range(0, nb * own, 32):
            rows = pl.ds(first, 32)
            dx = sx - tgx[rows, :]
            dy = sy - tgy[rows, :]
            dz = sz - tgz[rows, :]
            q = dx * dx + dy * dy + dz * dz + ss
            inverse = lax.rsqrt(q)
            interior = (q + q + ss) * (inverse * inverse)
            value = jnp.where(tgl[rows, :] > 0.5, interior, q) * inverse
            value_high, value_low = split(value)
            k_high[rows, columns(p)] = value_high
            k_low[rows, columns(p)] = value_low
        return carry

    lax.fori_loop(0, ng, kernel_block, 0)

    def weight_block(i, carry):
        p = lax.rem(g + i, ng)

        @pl.when(i > 0)
        def _():
            w_copy(p, p).wait_recv()

        w_high, w_low = split(weights[p])
        w_cat[0:systems, columns(p)] = w_high
        w_cat[systems : 2 * systems, columns(p)] = w_low
        return carry

    lax.fori_loop(0, ng, weight_block, 0)

    width = min(ng, 8) * own
    chunks = (ng * own) // width

    def product(c):
        cols = pl.ds(pl.multiple_of(c * width, width), width)
        both = nt_dot(w_cat[:, cols], k_high[:, cols])
        rest = nt_dot(w_cat[0:systems, cols], k_low[:, cols])
        return both[0:systems] + both[systems:] + rest

    if chunks == 1:
        total = product(0)
    else:
        acc[...] = jnp.zeros_like(acc)

        def add_chunk(c, carry):
            acc[...] += product(c)
            return carry

        lax.fori_loop(0, chunks, add_chunk, 0)
        total = acc[...]
    for k in range(nb):
        part[k] = total[:, k * own : (k + 1) * own]

    def img_copy(peer, slot):
        return remote(
            part.at[peer], part_in.at[slot], img_send.at[peer], img_recv.at[slot], (peer, g)
        )

    over(nb, 1, b, lambda p: img_copy(p, b).start())
    part_in[b] = part[b]
    over(nb, 1, b, lambda p: img_copy(p, p).wait_recv())
    image = part_in[0]
    for k in range(1, nb):
        image = image + part_in[k]
    image = image * (1.0 / math.sqrt(ndev * own))
    image_ref[...] = image

    image_high, image_low = split(image)
    image_cat = jnp.concatenate([image_high, image_low], axis=0)
    both = nt_dot(image_cat, sk_high[...])
    rest = nt_dot(image_high, sk_low[...])
    local = both[0:systems] + both[systems:] + rest
    for r in range(row_groups):
        for c in range(col_blocks):
            sk_part[r * col_blocks + c] = local[r * 8 : r * 8 + 8, c * 128 : c * 128 + 128]

    tile = lax.rem(me, tiles)
    base = me - tile

    def rs_copy(peer, slot):
        return remote(
            sk_part.at[lax.rem(peer, tiles)], sk_in.at[slot],
            rs_send.at[peer], rs_recv.at[slot], at(peer),
        )

    def ag_copy(peer, slot):
        return remote(
            sk_full.at[tile], sk_full.at[slot], ag_send.at[peer], ag_recv.at[slot], at(base + peer)
        )

    over(ndev, 1, me, lambda p: rs_copy(p, me).start())
    sk_in[me] = sk_part[tile]
    copies[5].wait()
    copies[6].wait()
    over(ndev, 1, me, lambda p: rs_copy(p, p).wait_recv())

    reach = min(ndev, 32)

    def add_tiles(i, value):
        for k in range(reach):
            value = value + sk_in[i * reach + k]
        return value

    if ndev == reach:
        summed = add_tiles(0, jnp.zeros((8, 128), F32))
    else:
        summed = lax.fori_loop(0, ndev // reach, add_tiles, jnp.zeros((8, 128), F32))
    sk_full[tile] = summed
    over(tiles, 1, tile, lambda p: ag_copy(p, tile).start())
    over(tiles, 1, tile, lambda p: ag_copy(p, p).wait_recv())

    lanes = lax.broadcasted_iota(jnp.int32, (8, 128), 1)
    for r in range(row_groups):
        rows = pl.ds(r * 8, 8)
        rest = [sk_full[r * col_blocks + c] for c in range(col_blocks)]
        coefs = []
        table = jnp.zeros((8, 128), F32)
        for j in range(vectors):
            run = rest[0] * basis[j, rows, 0:128]
            for c in range(1, col_blocks):
                run = run + rest[c] * basis[j, rows, c * 128 : c * 128 + 128]
            value = jnp.sum(run, axis=1, keepdims=True)
            coefs.append(value)
            table = jnp.where(lanes == j, value, table)
        squares = jnp.zeros((8, 128), F32)
        left = []
        for c in range(col_blocks):
            value = rest[c]
            for j in range(vectors):
                value = value - coefs[j] * basis[j, rows, c * 128 : c * 128 + 128]
            squares = squares + value * value
            left.append(value)
        mean = jnp.sum(squares, axis=1, keepdims=True) * (1.0 / (col_blocks * 128))
        norm = jnp.sqrt(mean + 1e-06)
        inverse = 1.0 / norm
        for c in range(col_blocks):
            sketch_next_ref[rows, c * 128 : c * 128 + 128] = left[c] * inverse
        vector = image_ref[rows, :]
        for j in range(vectors):
            vector = vector - coefs[j] * krylov[j, rows, :]
        next_ref[rows, :] = vector * inverse
        cmat[rows, :] = jnp.where(lanes == vectors, norm, table)
    turned = jnp.transpose(cmat[...])
    coef_ref[...] = turned[0:vectors, :]
    norms_ref[...] = turned[vectors : vectors + 1, :]

    over(nb, 1, b, lambda p: tgt_copy(p, b).wait_send())
    over(ng, 1, g, lambda p: geo_copy(p, g).wait_send())
    over(ng, 1, g, lambda p: w_copy(p, g).wait_send())
    over(nb, 1, b, lambda p: img_copy(p, b).wait_send())
    over(ndev, 1, me, lambda p: rs_copy(p, me).wait_send())
    over(tiles, 1, tile, lambda p: ag_copy(p, tile).wait_send())


def shards(nb, ng, points, labels, shape_scale, krylov_basis, sketch, sketched_basis):
    own = points.shape[1]
    vectors, systems, _ = krylov_basis.shape
    sketch_rows = sketch.shape[0]
    ndev = nb * ng
    tiles = (systems // 8) * (sketch_rows // 128)
    assert ndev % tiles == 0
    vmem = pltpu.VMEM
    dma = pltpu.SemaphoreType.DMA
    hbm = pl.BlockSpec(memory_space=pl.ANY)
    out = pl.BlockSpec(memory_space=pltpu.VMEM)
    next_vector, coefficients, sketch_next, norms = pl.pallas_call(
        functools.partial(step_kernel, nb, ng),
        out_shape=(
            jax.ShapeDtypeStruct((systems, own), F32),
            jax.ShapeDtypeStruct((vectors, systems), F32),
            jax.ShapeDtypeStruct((systems, sketch_rows), F32),
            jax.ShapeDtypeStruct((1, systems), F32),
        ),
        in_specs=[hbm] * 6,
        out_specs=(out,) * 4,
        scratch_shapes=[
            vmem((3, own), F32), vmem((1, own), jnp.int32), vmem((1, own), F32),
            vmem(krylov_basis.shape, F32), vmem(sketch.shape, F32), vmem(sketched_basis.shape, F32),
            vmem((8, own), F32), vmem((ng, 8, own), F32), vmem((nb, 8, own), F32),
            vmem((ng, systems, own), F32),
            vmem((nb * own, own), F32), vmem((nb * own, own), F32),
            vmem((nb * own, own), F32), vmem((nb * own, own), F32),
            vmem((nb * own, ng * own), BF16), vmem((nb * own, ng * own), BF16),
            vmem((2 * systems, ng * own), BF16), vmem((systems, nb * own), F32),
            vmem((nb, systems, own), F32), vmem((nb, systems, own), F32), vmem((systems, own), F32),
            vmem(sketch.shape, BF16), vmem(sketch.shape, BF16),
            vmem((tiles, 8, 128), F32), vmem((ndev, 8, 128), F32), vmem((tiles, 8, 128), F32),
            vmem((systems, 128), F32),
            dma((7,)), dma((ng,)), dma((ng,)), dma((ng,)), dma((ng,)), dma((nb,)), dma((nb,)),
            dma((nb,)), dma((nb,)), dma((ndev,)), dma((ndev,)), dma((tiles,)), dma((tiles,)),
        ],
        compiler_params=pltpu.CompilerParams(
            collective_id=0, has_side_effects=True, vmem_limit_bytes=48 * 1024 * 1024
        ),
    )(
        points, labels.reshape(1, own), shape_scale.reshape(1, own),
        krylov_basis, sketch, sketched_basis,
    )
    return (next_vector, coefficients, sketch_next, norms.reshape(systems))


def solution(mesh):
    placed = (
        P(None, ("blk", "grp")),
        P(("blk", "grp")),
        P(("blk", "grp")),
        P(None, None, ("blk", "grp")),
        P(None, ("blk", "grp")),
        P(),
    )
    return jax.shard_map(
        functools.partial(shards, mesh.shape["blk"], mesh.shape["grp"]),
        mesh=mesh,
        in_specs=placed,
        out_specs=(P(None, ("blk", "grp")), P(), P(), P()),
        check_vma=False,
    )
```

```python
import functools
import math

import jax
import jax.numpy as jnp
from jax import lax
from jax.experimental import pallas as pl
from jax.experimental.pallas import tpu as pltpu
from jax.sharding import PartitionSpec as P

MESH = pl.DeviceIdType.MESH
F32 = jnp.float32
BF16 = jnp.bfloat16
NT = (((1,), (1,)), ((), ()))


def split(value):
    high = value.astype(BF16)
    low = (value - high.astype(F32)).astype(BF16)
    return high, low


def nt_dot(left, right):
    return lax.dot_general(left, right, NT, preferred_element_type=F32)


def step_kernel(
    nb, ng,
    points_hbm, labels_hbm, scale_hbm, krylov_hbm, sketch_hbm, basis_hbm,
    next_ref, coef_ref, sketch_next_ref, norms_ref,
    pts, lab, scl, krylov, sketch, basis,
    geo, src_geo, tgt_geo, weights,
    tgx, tgy, tgz, tgl, k_high, k_low, w_cat, acc,
    part, part_in, image_ref, sk_high, sk_low,
    sk_part, sk_in, sk_full, cmat,
    local_sem, geo_send, geo_recv, w_send, w_recv, tgt_send, tgt_recv,
    img_send, img_recv, rs_send, rs_recv, ag_send, ag_recv,
):
    b = lax.axis_index("blk")
    g = lax.axis_index("grp")
    ndev = nb * ng
    me = b * ng + g
    own = pts.shape[1]
    vectors, systems, _ = krylov.shape
    tiles = sk_part.shape[0]
    row_groups = systems // 8
    col_blocks = tiles // row_groups

    def at(d):
        return (d // ng, lax.rem(d, ng))

    def remote(src, dst, send, recv, where):
        return pltpu.make_async_remote_copy(
            src_ref=src, dst_ref=dst, send_sem=send, recv_sem=recv,
            device_id=where, device_id_type=MESH,
        )

    copies = [
        pltpu.make_async_copy(points_hbm, pts, local_sem.at[0]),
        pltpu.make_async_copy(labels_hbm, lab, local_sem.at[1]),
        pltpu.make_async_copy(scale_hbm, scl, local_sem.at[2]),
        pltpu.make_async_copy(krylov_hbm.at[vectors - 1], weights.at[g], local_sem.at[3]),
        pltpu.make_async_copy(sketch_hbm, sketch, local_sem.at[4]),
        pltpu.make_async_copy(krylov_hbm, krylov, local_sem.at[5]),
        pltpu.make_async_copy(basis_hbm, basis, local_sem.at[6]),
    ]
    for copy in copies:
        copy.start()

    barrier = pltpu.get_barrier_semaphore()

    def over(count, first, self_index, action):
        def step(i, carry):
            action(lax.rem(self_index + i, count))
            return carry

        lax.fori_loop(first, count, step, 0)

    def greet(where):
        pl.semaphore_signal(barrier, inc=1, device_id=where, device_id_type=MESH)

    over(ng, 1, g, lambda p: greet((b, p)))
    over(nb, 1, b, lambda p: greet((p, g)))

    for copy in copies[:3]:
        copy.wait()
    scale = scl[...]
    mine = jnp.concatenate(
        [pts[...], scale * scale, lab[...].astype(F32), jnp.zeros((3, own), F32)], axis=0
    )
    geo[...] = mine
    src_geo[g] = mine
    tgt_geo[b] = mine
    copies[4].wait()
    high, low = split(sketch[...])
    sk_high[...] = high
    sk_low[...] = low
    copies[3].wait()
    pl.semaphore_wait(barrier, ng + nb - 2)

    def geo_copy(peer, slot):
        return remote(geo, src_geo.at[slot], geo_send.at[peer], geo_recv.at[slot], (b, peer))

    def tgt_copy(peer, slot):
        return remote(geo, tgt_geo.at[slot], tgt_send.at[peer], tgt_recv.at[slot], (peer, g))

    def w_copy(peer, slot):
        return remote(
            weights.at[g], weights.at[slot], w_send.at[peer], w_recv.at[slot], (b, peer)
        )

    over(nb, 1, b, lambda p: tgt_copy(p, b).start())
    over(ng, 1, g, lambda p: geo_copy(p, g).start())
    over(ng, 1, g, lambda p: w_copy(p, g).start())

    over(nb, 1, b, lambda p: tgt_copy(p, p).wait_recv())
    for k in range(nb):
        turned = jnp.transpose(tgt_geo[k])
        rows = pl.ds(k * own, own)
        tgx[rows, :] = jnp.broadcast_to(turned[:, 0:1], (own, own))
        tgy[rows, :] = jnp.broadcast_to(turned[:, 1:2], (own, own))
        tgz[rows, :] = jnp.broadcast_to(turned[:, 2:3], (own, own))
        tgl[rows, :] = jnp.broadcast_to(turned[:, 4:5], (own, own))

    def columns(p):
        return pl.ds(pl.multiple_of(p * own, own), own)

    def kernel_block(i, carry):
        p = lax.rem(g + i, ng)

        @pl.when(i > 0)
        def _():
            geo_copy(p, p).wait_recv()

        block = src_geo[p]
        sx, sy, sz, ss = block[0:1], block[1:2], block[2:3], block[3:4]
        for first in range(0, nb * own, 32):
            rows = pl.ds(first, 32)
            dx = sx - tgx[rows, :]
            dy = sy - tgy[rows, :]
            dz = sz - tgz[rows, :]
            q = dx * dx + dy * dy + dz * dz + ss
            inverse = lax.rsqrt(q)
            interior = (q + q + ss) * (inverse * inverse)
            value = jnp.where(tgl[rows, :] > 0.5, interior, q) * inverse
            value_high, value_low = split(value)
            k_high[rows, columns(p)] = value_high
            k_low[rows, columns(p)] = value_low
        return carry

    lax.fori_loop(0, ng, kernel_block, 0)

    def weight_block(i, carry):
        p = lax.rem(g + i, ng)

        @pl.when(i > 0)
        def _():
            w_copy(p, p).wait_recv()

        w_high, w_low = split(weights[p])
        w_cat[0:systems, columns(p)] = w_high
        w_cat[systems : 2 * systems, columns(p)] = w_low
        return carry

    lax.fori_loop(0, ng, weight_block, 0)

    width = min(ng, 8) * own
    chunks = (ng * own) // width

    def product(c):
        cols = pl.ds(pl.multiple_of(c * width, width), width)
        both = nt_dot(w_cat[:, cols], k_high[:, cols])
        rest = nt_dot(w_cat[0:systems, cols], k_low[:, cols])
        return both[0:systems] + both[systems:] + rest

    if chunks == 1:
        total = product(0)
    else:
        acc[...] = jnp.zeros_like(acc)

        def add_chunk(c, carry):
            acc[...] += product(c)
            return carry

        lax.fori_loop(0, chunks, add_chunk, 0)
        total = acc[...]
    for k in range(nb):
        part[k] = total[:, k * own : (k + 1) * own]

    def img_copy(peer, slot):
        return remote(
            part.at[peer], part_in.at[slot], img_send.at[peer], img_recv.at[slot], (peer, g)
        )

    over(nb, 1, b, lambda p: img_copy(p, b).start())
    part_in[b] = part[b]
    over(nb, 1, b, lambda p: img_copy(p, p).wait_recv())
    image = part_in[0]
    for k in range(1, nb):
        image = image + part_in[k]
    image = image * (1.0 / math.sqrt(ndev * own))
    image_ref[...] = image

    image_high, image_low = split(image)
    image_cat = jnp.concatenate([image_high, image_low], axis=0)
    both = nt_dot(image_cat, sk_high[...])
    rest = nt_dot(image_high, sk_low[...])
    local = both[0:systems] + both[systems:] + rest
    for r in range(row_groups):
        for c in range(col_blocks):
            sk_part[r * col_blocks + c] = local[r * 8 : r * 8 + 8, c * 128 : c * 128 + 128]

    tile = lax.rem(me, tiles)
    base = me - tile

    def rs_copy(peer, slot):
        return remote(
            sk_part.at[lax.rem(peer, tiles)], sk_in.at[slot],
            rs_send.at[peer], rs_recv.at[slot], at(peer),
        )

    def ag_copy(peer, slot):
        return remote(
            sk_full.at[tile], sk_full.at[slot], ag_send.at[peer], ag_recv.at[slot], at(base + peer)
        )

    def far_first(count, width, index, action):
        low = lax.rem(index, width) < width // 2

        def step(i, carry):
            along = i // (count // width)
            other = lax.rem(i, count // width)
            p = other * width + jnp.where(low, width - 1 - along, along)

            @pl.when(p != index)
            def _():
                action(p)

            return carry

        lax.fori_loop(0, count, step, 0)

    far_first(ndev, ng, me, lambda p: rs_copy(p, me).start())
    sk_in[me] = sk_part[tile]
    copies[5].wait()
    copies[6].wait()
    over(ndev, 1, me, lambda p: rs_copy(p, p).wait_recv())

    reach = min(ndev, 32)

    def add_tiles(i, value):
        for k in range(reach):
            value = value + sk_in[i * reach + k]
        return value

    if ndev == reach:
        summed = add_tiles(0, jnp.zeros((8, 128), F32))
    else:
        summed = lax.fori_loop(0, ndev // reach, add_tiles, jnp.zeros((8, 128), F32))
    sk_full[tile] = summed
    far_first(tiles, min(ng, tiles), tile, lambda p: ag_copy(p, tile).start())
    over(tiles, 1, tile, lambda p: ag_copy(p, p).wait_recv())

    lanes = lax.broadcasted_iota(jnp.int32, (8, 128), 1)
    for r in range(row_groups):
        rows = pl.ds(r * 8, 8)
        rest = [sk_full[r * col_blocks + c] for c in range(col_blocks)]
        coefs = []
        table = jnp.zeros((8, 128), F32)
        for j in range(vectors):
            run = rest[0] * basis[j, rows, 0:128]
            for c in range(1, col_blocks):
                run = run + rest[c] * basis[j, rows, c * 128 : c * 128 + 128]
            value = jnp.sum(run, axis=1, keepdims=True)
            coefs.append(value)
            table = jnp.where(lanes == j, value, table)
        squares = jnp.zeros((8, 128), F32)
        left = []
        for c in range(col_blocks):
            value = rest[c]
            for j in range(vectors):
                value = value - coefs[j] * basis[j, rows, c * 128 : c * 128 + 128]
            squares = squares + value * value
            left.append(value)
        mean = jnp.sum(squares, axis=1, keepdims=True) * (1.0 / (col_blocks * 128))
        norm = jnp.sqrt(mean + 1e-06)
        inverse = 1.0 / norm
        for c in range(col_blocks):
            sketch_next_ref[rows, c * 128 : c * 128 + 128] = left[c] * inverse
        vector = image_ref[rows, :]
        for j in range(vectors):
            vector = vector - coefs[j] * krylov[j, rows, :]
        next_ref[rows, :] = vector * inverse
        cmat[rows, :] = jnp.where(lanes == vectors, norm, table)
    turned = jnp.transpose(cmat[...])
    coef_ref[...] = turned[0:vectors, :]
    norms_ref[...] = turned[vectors : vectors + 1, :]

    over(nb, 1, b, lambda p: tgt_copy(p, b).wait_send())
    over(ng, 1, g, lambda p: geo_copy(p, g).wait_send())
    over(ng, 1, g, lambda p: w_copy(p, g).wait_send())
    over(nb, 1, b, lambda p: img_copy(p, b).wait_send())
    over(ndev, 1, me, lambda p: rs_copy(p, me).wait_send())
    over(tiles, 1, tile, lambda p: ag_copy(p, tile).wait_send())


def place_kernel(count, *refs):
    sems = refs[2 * count]
    outward = [pltpu.make_async_copy(refs[k], refs[count + k], sems.at[k]) for k in range(count)]
    for copy in outward:
        copy.start()
    for copy in outward:
        copy.wait()


def place(arrays):
    count = len(arrays)
    return pl.pallas_call(
        functools.partial(place_kernel, count),
        out_shape=tuple(jax.ShapeDtypeStruct(a.shape, a.dtype) for a in arrays),
        in_specs=[pl.BlockSpec(memory_space=pltpu.VMEM)] * count,
        out_specs=(pl.BlockSpec(memory_space=pltpu.HBM),) * count,
        scratch_shapes=[pltpu.SemaphoreType.DMA((count,))],
        compiler_params=pltpu.CompilerParams(vmem_limit_bytes=1024 * 1024),
    )(*arrays)


def shards(nb, ng, points, labels, shape_scale, krylov_basis, sketch, sketched_basis):
    own = points.shape[1]
    vectors, systems, _ = krylov_basis.shape
    sketch_rows = sketch.shape[0]
    ndev = nb * ng
    tiles = (systems // 8) * (sketch_rows // 128)
    assert ndev % tiles == 0
    vmem = pltpu.VMEM
    dma = pltpu.SemaphoreType.DMA
    hbm = pl.BlockSpec(memory_space=pltpu.HBM)
    out = pl.BlockSpec(memory_space=pltpu.VMEM)
    operands = [
        pltpu.with_memory_space_constraint(operand, pltpu.HBM)
        for operand in (
            points, labels.reshape(1, own), shape_scale.reshape(1, own),
            krylov_basis, sketch, sketched_basis,
        )
    ]
    results = pl.pallas_call(
        functools.partial(step_kernel, nb, ng),
        out_shape=(
            jax.ShapeDtypeStruct((systems, own), F32),
            jax.ShapeDtypeStruct((vectors, systems), F32),
            jax.ShapeDtypeStruct((systems, sketch_rows), F32),
            jax.ShapeDtypeStruct((1, systems), F32),
        ),
        in_specs=[hbm] * 6,
        out_specs=(out,) * 4,
        scratch_shapes=[
            vmem((3, own), F32), vmem((1, own), jnp.int32), vmem((1, own), F32),
            vmem(krylov_basis.shape, F32), vmem(sketch.shape, F32), vmem(sketched_basis.shape, F32),
            vmem((8, own), F32), vmem((ng, 8, own), F32), vmem((nb, 8, own), F32),
            vmem((ng, systems, own), F32),
            vmem((nb * own, own), F32), vmem((nb * own, own), F32),
            vmem((nb * own, own), F32), vmem((nb * own, own), F32),
            vmem((nb * own, ng * own), BF16), vmem((nb * own, ng * own), BF16),
            vmem((2 * systems, ng * own), BF16), vmem((systems, nb * own), F32),
            vmem((nb, systems, own), F32), vmem((nb, systems, own), F32), vmem((systems, own), F32),
            vmem(sketch.shape, BF16), vmem(sketch.shape, BF16),
            vmem((tiles, 8, 128), F32), vmem((ndev, 8, 128), F32), vmem((tiles, 8, 128), F32),
            vmem((systems, 128), F32),
            dma((7,)), dma((ng,)), dma((ng,)), dma((ng,)), dma((ng,)), dma((nb,)), dma((nb,)),
            dma((nb,)), dma((nb,)), dma((ndev,)), dma((ndev,)), dma((tiles,)), dma((tiles,)),
        ],
        compiler_params=pltpu.CompilerParams(
            collective_id=0, has_side_effects=True, vmem_limit_bytes=48 * 1024 * 1024
        ),
    )(*operands)
    next_vector, coefficients, sketch_next, norms = place(results)
    return (next_vector, coefficients, sketch_next, norms.reshape(systems))


def solution(mesh):
    placed = (
        P(None, ("blk", "grp")),
        P(("blk", "grp")),
        P(("blk", "grp")),
        P(None, None, ("blk", "grp")),
        P(None, ("blk", "grp")),
        P(),
    )
    return jax.shard_map(
        functools.partial(shards, mesh.shape["blk"], mesh.shape["grp"]),
        mesh=mesh,
        in_specs=placed,
        out_specs=(P(None, ("blk", "grp")), P(), P(), P()),
        check_vma=False,
    )
```

```python
import functools
import math

import jax
import jax.numpy as jnp
from jax import lax
from jax.experimental import pallas as pl
from jax.experimental.pallas import tpu as pltpu
from jax.sharding import PartitionSpec as P

MESH = pl.DeviceIdType.MESH
F32 = jnp.float32
BF16 = jnp.bfloat16
NT = (((1,), (1,)), ((), ()))


def split(value):
    high = value.astype(BF16)
    low = (value - high.astype(F32)).astype(BF16)
    return high, low


def nt_dot(left, right):
    return lax.dot_general(left, right, NT, preferred_element_type=F32)


def step_kernel(
    nb, ng,
    points_hbm, labels_hbm, scale_hbm, krylov_hbm, sketch_hbm, basis_hbm,
    next_ref, coef_ref, sketch_next_ref, norms_ref,
    pts, lab, scl, krylov, sketch, basis,
    geo, src_geo, tgt_geo, weights,
    tgx, tgy, tgz, tgl, k_high, k_low, w_cat, acc,
    part, part_in, image_ref, sk_high, sk_low,
    sk_part, sk_in, sk_full, cmat,
    local_sem, geo_send, geo_recv, w_send, w_recv, tgt_send, tgt_recv,
    img_send, img_recv, rs_send, rs_recv, ag_send, ag_recv,
):
    b = lax.axis_index("blk")
    g = lax.axis_index("grp")
    ndev = nb * ng
    me = b * ng + g
    own = pts.shape[1]
    vectors, systems, _ = krylov.shape
    tiles = sk_part.shape[0]
    row_groups = systems // 8
    col_blocks = tiles // row_groups

    def at(d):
        return (d // ng, lax.rem(d, ng))

    def remote(src, dst, send, recv, where):
        return pltpu.make_async_remote_copy(
            src_ref=src, dst_ref=dst, send_sem=send, recv_sem=recv,
            device_id=where, device_id_type=MESH,
        )

    copies = [
        pltpu.make_async_copy(points_hbm, pts, local_sem.at[0]),
        pltpu.make_async_copy(labels_hbm, lab, local_sem.at[1]),
        pltpu.make_async_copy(scale_hbm, scl, local_sem.at[2]),
        pltpu.make_async_copy(krylov_hbm.at[vectors - 1], weights.at[g], local_sem.at[3]),
        pltpu.make_async_copy(sketch_hbm, sketch, local_sem.at[4]),
        pltpu.make_async_copy(krylov_hbm, krylov, local_sem.at[5]),
        pltpu.make_async_copy(basis_hbm, basis, local_sem.at[6]),
    ]
    for copy in copies:
        copy.start()

    barrier = pltpu.get_barrier_semaphore()

    def over(count, first, self_index, action):
        def step(i, carry):
            action(lax.rem(self_index + i, count))
            return carry

        lax.fori_loop(first, count, step, 0)

    def greet(where):
        pl.semaphore_signal(barrier, inc=1, device_id=where, device_id_type=MESH)

    over(ng, 1, g, lambda p: greet((b, p)))
    over(nb, 1, b, lambda p: greet((p, g)))

    for copy in copies[:3]:
        copy.wait()
    scale = scl[...]
    mine = jnp.concatenate(
        [pts[...], scale * scale, lab[...].astype(F32), jnp.zeros((3, own), F32)], axis=0
    )
    geo[...] = mine
    src_geo[g] = mine
    tgt_geo[b] = mine
    copies[3].wait()
    pl.semaphore_wait(barrier, ng + nb - 2)

    def geo_copy(peer, slot):
        return remote(geo, src_geo.at[slot], geo_send.at[peer], geo_recv.at[slot], (b, peer))

    def tgt_copy(peer, slot):
        return remote(geo, tgt_geo.at[slot], tgt_send.at[peer], tgt_recv.at[slot], (peer, g))

    def w_copy(peer, slot):
        return remote(
            weights.at[g], weights.at[slot], w_send.at[peer], w_recv.at[slot], (b, peer)
        )

    def far_first(count, width, index, action):
        low = lax.rem(index, width) < width // 2

        def step(i, carry):
            along = i // (count // width)
            other = lax.rem(i, count // width)
            p = other * width + jnp.where(low, width - 1 - along, along)

            @pl.when(p != index)
            def _():
                action(p)

            return carry

        lax.fori_loop(0, count, step, 0)

    over(nb, 1, b, lambda p: tgt_copy(p, b).start())
    far_first(ng, ng, g, lambda p: geo_copy(p, g).start())
    far_first(ng, ng, g, lambda p: w_copy(p, g).start())

    copies[4].wait()
    high, low = split(sketch[...])
    sk_high[...] = high
    sk_low[...] = low
    over(nb, 1, b, lambda p: tgt_copy(p, p).wait_recv())
    for k in range(nb):
        turned = jnp.transpose(tgt_geo[k])
        rows = pl.ds(k * own, own)
        tgx[rows, :] = jnp.broadcast_to(turned[:, 0:1], (own, own))
        tgy[rows, :] = jnp.broadcast_to(turned[:, 1:2], (own, own))
        tgz[rows, :] = jnp.broadcast_to(turned[:, 2:3], (own, own))
        tgl[rows, :] = jnp.broadcast_to(turned[:, 4:5], (own, own))

    def columns(p):
        return pl.ds(pl.multiple_of(p * own, own), own)

    def kernel_block(i, carry):
        p = jnp.where(g < ng // 2, i, ng - 1 - i)

        @pl.when(p != g)
        def _():
            geo_copy(p, p).wait_recv()

        block = src_geo[p]
        sx, sy, sz, ss = block[0:1], block[1:2], block[2:3], block[3:4]
        for first in range(0, nb * own, 32):
            rows = pl.ds(first, 32)
            dx = sx - tgx[rows, :]
            dy = sy - tgy[rows, :]
            dz = sz - tgz[rows, :]
            q = dx * dx + dy * dy + dz * dz + ss
            inverse = lax.rsqrt(q)
            interior = (q + q + ss) * (inverse * inverse)
            value = jnp.where(tgl[rows, :] > 0.5, interior, q) * inverse
            value_high, value_low = split(value)
            k_high[rows, columns(i)] = value_high
            k_low[rows, columns(i)] = value_low
        return carry

    lax.fori_loop(0, ng, kernel_block, 0)

    def weight_block(i, carry):
        p = jnp.where(g < ng // 2, i, ng - 1 - i)

        @pl.when(p != g)
        def _():
            w_copy(p, p).wait_recv()

        w_high, w_low = split(weights[p])
        w_cat[0:systems, columns(i)] = w_high
        w_cat[systems : 2 * systems, columns(i)] = w_low
        return carry

    batch = min(ng // 2, 8)
    width = batch * own

    def product(c):
        lax.fori_loop(c * batch, (c + 1) * batch, weight_block, 0)
        cols = pl.ds(pl.multiple_of(c * width, width), width)
        both = nt_dot(w_cat[:, cols], k_high[:, cols])
        rest = nt_dot(w_cat[0:systems, cols], k_low[:, cols])
        return both[0:systems] + both[systems:] + rest

    acc[...] = product(0)
    if ng // batch > 2:

        def add_chunk(c, carry):
            acc[...] += product(c)
            return carry

        lax.fori_loop(1, ng // batch - 1, add_chunk, 0)
    total = acc[...] + product(ng // batch - 1)
    for k in range(nb):
        part[k] = total[:, k * own : (k + 1) * own]

    def img_copy(peer, slot):
        return remote(
            part.at[peer], part_in.at[slot], img_send.at[peer], img_recv.at[slot], (peer, g)
        )

    over(nb, 1, b, lambda p: img_copy(p, b).start())
    part_in[b] = part[b]
    over(nb, 1, b, lambda p: img_copy(p, p).wait_recv())
    image = part_in[0]
    for k in range(1, nb):
        image = image + part_in[k]
    image = image * (1.0 / math.sqrt(ndev * own))
    image_ref[...] = image

    image_high, image_low = split(image)
    image_cat = jnp.concatenate([image_high, image_low], axis=0)
    both = nt_dot(image_cat, sk_high[...])
    rest = nt_dot(image_high, sk_low[...])
    local = both[0:systems] + both[systems:] + rest
    for r in range(row_groups):
        for c in range(col_blocks):
            sk_part[r * col_blocks + c] = local[r * 8 : r * 8 + 8, c * 128 : c * 128 + 128]

    tile = lax.rem(me, tiles)
    base = me - tile

    def rs_copy(peer, slot):
        return remote(
            sk_part.at[lax.rem(peer, tiles)], sk_in.at[slot],
            rs_send.at[peer], rs_recv.at[slot], at(peer),
        )

    def ag_copy(peer, slot):
        return remote(
            sk_full.at[tile], sk_full.at[slot], ag_send.at[peer], ag_recv.at[slot], at(base + peer)
        )

    far_first(ndev, ng, me, lambda p: rs_copy(p, me).start())
    sk_in[me] = sk_part[tile]
    copies[5].wait()
    copies[6].wait()
    over(ndev, 1, me, lambda p: rs_copy(p, p).wait_recv())

    reach = min(ndev, 32)

    def add_tiles(i, value):
        for k in range(reach):
            value = value + sk_in[i * reach + k]
        return value

    if ndev == reach:
        summed = add_tiles(0, jnp.zeros((8, 128), F32))
    else:
        summed = lax.fori_loop(0, ndev // reach, add_tiles, jnp.zeros((8, 128), F32))
    sk_full[tile] = summed
    far_first(tiles, min(ng, tiles), tile, lambda p: ag_copy(p, tile).start())
    over(tiles, 1, tile, lambda p: ag_copy(p, p).wait_recv())

    lanes = lax.broadcasted_iota(jnp.int32, (8, 128), 1)
    for r in range(row_groups):
        rows = pl.ds(r * 8, 8)
        rest = [sk_full[r * col_blocks + c] for c in range(col_blocks)]
        coefs = []
        table = jnp.zeros((8, 128), F32)
        for j in range(vectors):
            run = rest[0] * basis[j, rows, 0:128]
            for c in range(1, col_blocks):
                run = run + rest[c] * basis[j, rows, c * 128 : c * 128 + 128]
            value = jnp.sum(run, axis=1, keepdims=True)
            coefs.append(value)
            table = jnp.where(lanes == j, value, table)
        squares = jnp.zeros((8, 128), F32)
        left = []
        for c in range(col_blocks):
            value = rest[c]
            for j in range(vectors):
                value = value - coefs[j] * basis[j, rows, c * 128 : c * 128 + 128]
            squares = squares + value * value
            left.append(value)
        mean = jnp.sum(squares, axis=1, keepdims=True) * (1.0 / (col_blocks * 128))
        norm = jnp.sqrt(mean + 1e-06)
        inverse = 1.0 / norm
        for c in range(col_blocks):
            sketch_next_ref[rows, c * 128 : c * 128 + 128] = left[c] * inverse
        vector = image_ref[rows, :]
        for j in range(vectors):
            vector = vector - coefs[j] * krylov[j, rows, :]
        next_ref[rows, :] = vector * inverse
        cmat[rows, :] = jnp.where(lanes == vectors, norm, table)
    turned = jnp.transpose(cmat[...])
    coef_ref[...] = turned[0:vectors, :]
    norms_ref[...] = turned[vectors : vectors + 1, :]

    over(nb, 1, b, lambda p: tgt_copy(p, b).wait_send())
    over(ng, 1, g, lambda p: geo_copy(p, g).wait_send())
    over(ng, 1, g, lambda p: w_copy(p, g).wait_send())
    over(nb, 1, b, lambda p: img_copy(p, b).wait_send())
    over(ndev, 1, me, lambda p: rs_copy(p, me).wait_send())
    over(tiles, 1, tile, lambda p: ag_copy(p, tile).wait_send())


def place_kernel(count, *refs):
    sems = refs[2 * count]
    outward = [pltpu.make_async_copy(refs[k], refs[count + k], sems.at[k]) for k in range(count)]
    for copy in outward:
        copy.start()
    for copy in outward:
        copy.wait()


def place(arrays):
    count = len(arrays)
    return pl.pallas_call(
        functools.partial(place_kernel, count),
        out_shape=tuple(jax.ShapeDtypeStruct(a.shape, a.dtype) for a in arrays),
        in_specs=[pl.BlockSpec(memory_space=pltpu.VMEM)] * count,
        out_specs=(pl.BlockSpec(memory_space=pltpu.HBM),) * count,
        scratch_shapes=[pltpu.SemaphoreType.DMA((count,))],
        compiler_params=pltpu.CompilerParams(vmem_limit_bytes=1024 * 1024),
    )(*arrays)


def shards(nb, ng, points, labels, shape_scale, krylov_basis, sketch, sketched_basis):
    own = points.shape[1]
    vectors, systems, _ = krylov_basis.shape
    sketch_rows = sketch.shape[0]
    ndev = nb * ng
    tiles = (systems // 8) * (sketch_rows // 128)
    assert ndev % tiles == 0
    vmem = pltpu.VMEM
    dma = pltpu.SemaphoreType.DMA
    hbm = pl.BlockSpec(memory_space=pltpu.HBM)
    out = pl.BlockSpec(memory_space=pltpu.VMEM)
    operands = [
        pltpu.with_memory_space_constraint(operand, pltpu.HBM)
        for operand in (
            points, labels.reshape(1, own), shape_scale.reshape(1, own),
            krylov_basis, sketch, sketched_basis,
        )
    ]
    results = pl.pallas_call(
        functools.partial(step_kernel, nb, ng),
        out_shape=(
            jax.ShapeDtypeStruct((systems, own), F32),
            jax.ShapeDtypeStruct((vectors, systems), F32),
            jax.ShapeDtypeStruct((systems, sketch_rows), F32),
            jax.ShapeDtypeStruct((1, systems), F32),
        ),
        in_specs=[hbm] * 6,
        out_specs=(out,) * 4,
        scratch_shapes=[
            vmem((3, own), F32), vmem((1, own), jnp.int32), vmem((1, own), F32),
            vmem(krylov_basis.shape, F32), vmem(sketch.shape, F32), vmem(sketched_basis.shape, F32),
            vmem((8, own), F32), vmem((ng, 8, own), F32), vmem((nb, 8, own), F32),
            vmem((ng, systems, own), F32),
            vmem((nb * own, own), F32), vmem((nb * own, own), F32),
            vmem((nb * own, own), F32), vmem((nb * own, own), F32),
            vmem((nb * own, ng * own), BF16), vmem((nb * own, ng * own), BF16),
            vmem((2 * systems, ng * own), BF16), vmem((systems, nb * own), F32),
            vmem((nb, systems, own), F32), vmem((nb, systems, own), F32), vmem((systems, own), F32),
            vmem(sketch.shape, BF16), vmem(sketch.shape, BF16),
            vmem((tiles, 8, 128), F32), vmem((ndev, 8, 128), F32), vmem((tiles, 8, 128), F32),
            vmem((systems, 128), F32),
            dma((7,)), dma((ng,)), dma((ng,)), dma((ng,)), dma((ng,)), dma((nb,)), dma((nb,)),
            dma((nb,)), dma((nb,)), dma((ndev,)), dma((ndev,)), dma((tiles,)), dma((tiles,)),
        ],
        compiler_params=pltpu.CompilerParams(
            collective_id=0, has_side_effects=True, vmem_limit_bytes=48 * 1024 * 1024
        ),
    )(*operands)
    next_vector, coefficients, sketch_next, norms = place(results)
    return (next_vector, coefficients, sketch_next, norms.reshape(systems))


def solution(mesh):
    placed = (
        P(None, ("blk", "grp")),
        P(("blk", "grp")),
        P(("blk", "grp")),
        P(None, None, ("blk", "grp")),
        P(None, ("blk", "grp")),
        P(),
    )
    return jax.shard_map(
        functools.partial(shards, mesh.shape["blk"], mesh.shape["grp"]),
        mesh=mesh,
        in_specs=placed,
        out_specs=(P(None, ("blk", "grp")), P(), P(), P()),
        check_vma=False,
    )
```

```python
import functools
import math

import jax
import jax.numpy as jnp
from jax import lax
from jax.experimental import pallas as pl
from jax.experimental.pallas import tpu as pltpu
from jax.sharding import PartitionSpec as P

MESH = pl.DeviceIdType.MESH
F32 = jnp.float32
BF16 = jnp.bfloat16
NT = (((1,), (1,)), ((), ()))


def split(value):
    high = value.astype(BF16)
    low = (value - high.astype(F32)).astype(BF16)
    return high, low


def nt_dot(left, right):
    return lax.dot_general(left, right, NT, preferred_element_type=F32)


def step_kernel(
    nb, ng,
    points_hbm, labels_hbm, scale_hbm, krylov_hbm, sketch_hbm, basis_hbm,
    next_ref, coef_ref, sketch_next_ref, norms_ref,
    pts, lab, scl, krylov, sketch, basis,
    geo, src_geo, tgt_geo, weights,
    tgx, tgy, tgz, tgl, k_high, k_low, w_cat, acc,
    part, part_in, image_ref, sk_high, sk_low,
    sk_part, sk_in, sk_full, cmat,
    local_sem, geo_send, geo_recv, w_send, w_recv, tgt_send, tgt_recv,
    img_send, img_recv, rs_send, rs_recv, ag_send, ag_recv,
):
    b = lax.axis_index("blk")
    g = lax.axis_index("grp")
    ndev = nb * ng
    me = b * ng + g
    own = pts.shape[1]
    vectors, systems, _ = krylov.shape
    tiles = sk_part.shape[0]
    row_groups = systems // 8
    col_blocks = tiles // row_groups

    def at(d):
        return (d // ng, lax.rem(d, ng))

    def remote(src, dst, send, recv, where):
        return pltpu.make_async_remote_copy(
            src_ref=src, dst_ref=dst, send_sem=send, recv_sem=recv,
            device_id=where, device_id_type=MESH,
        )

    copies = [
        pltpu.make_async_copy(points_hbm, pts, local_sem.at[0]),
        pltpu.make_async_copy(labels_hbm, lab, local_sem.at[1]),
        pltpu.make_async_copy(scale_hbm, scl, local_sem.at[2]),
        pltpu.make_async_copy(krylov_hbm.at[vectors - 1], weights.at[g], local_sem.at[3]),
        pltpu.make_async_copy(sketch_hbm, sketch, local_sem.at[4]),
        pltpu.make_async_copy(krylov_hbm, krylov, local_sem.at[5]),
        pltpu.make_async_copy(basis_hbm, basis, local_sem.at[6]),
    ]
    barrier = pltpu.get_barrier_semaphore()

    def over(count, first, self_index, action):
        def step(i, carry):
            action(lax.rem(self_index + i, count))
            return carry

        lax.fori_loop(first, count, step, 0, unroll=count <= 32)

    def greet(where):
        pl.semaphore_signal(barrier, inc=1, device_id=where, device_id_type=MESH)

    over(ng, 1, g, lambda p: greet((b, p)))
    over(nb, 1, b, lambda p: greet((p, g)))
    for copy in copies:
        copy.start()

    for copy in copies[:3]:
        copy.wait()
    scale = scl[...]
    mine = jnp.concatenate(
        [pts[...], scale * scale, lab[...].astype(F32), jnp.zeros((3, own), F32)], axis=0
    )
    geo[...] = mine
    src_geo[g] = mine
    tgt_geo[b] = mine
    copies[3].wait()
    pl.semaphore_wait(barrier, ng + nb - 2)

    def geo_copy(peer, slot):
        return remote(geo, src_geo.at[slot], geo_send.at[peer], geo_recv.at[slot], (b, peer))

    def tgt_copy(peer, slot):
        return remote(geo, tgt_geo.at[slot], tgt_send.at[peer], tgt_recv.at[slot], (peer, g))

    def w_copy(peer, slot):
        return remote(
            weights.at[g], weights.at[slot], w_send.at[peer], w_recv.at[slot], (b, peer)
        )

    def far_first(count, width, index, action):
        low = lax.rem(index, width) < width // 2

        def step(i, carry):
            along = i // (count // width)
            other = lax.rem(i, count // width)
            p = other * width + jnp.where(low, width - 1 - along, along)

            @pl.when(p != index)
            def _():
                action(p)

            return carry

        lax.fori_loop(0, count, step, 0, unroll=count <= 32)

    over(nb, 1, b, lambda p: tgt_copy(p, b).start())
    far_first(ng, ng, g, lambda p: geo_copy(p, g).start())
    far_first(ng, ng, g, lambda p: w_copy(p, g).start())

    copies[4].wait()
    high, low = split(sketch[...])
    sk_high[...] = high
    sk_low[...] = low
    over(nb, 1, b, lambda p: tgt_copy(p, p).wait_recv())
    for k in range(nb):
        turned = jnp.transpose(tgt_geo[k])
        rows = pl.ds(k * own, own)
        tgx[rows, :] = jnp.broadcast_to(turned[:, 0:1], (own, own))
        tgy[rows, :] = jnp.broadcast_to(turned[:, 1:2], (own, own))
        tgz[rows, :] = jnp.broadcast_to(turned[:, 2:3], (own, own))
        tgl[rows, :] = jnp.broadcast_to(turned[:, 4:5], (own, own))

    def columns(p):
        return pl.ds(pl.multiple_of(p * own, own), own)

    def kernel_block(i, carry):
        p = jnp.where(g < ng // 2, i, ng - 1 - i)

        @pl.when(p != g)
        def _():
            geo_copy(p, p).wait_recv()

        block = src_geo[p]
        sx, sy, sz, ss = block[0:1], block[1:2], block[2:3], block[3:4]
        for first in range(0, nb * own, 32):
            rows = pl.ds(first, 32)
            dx = sx - tgx[rows, :]
            dy = sy - tgy[rows, :]
            dz = sz - tgz[rows, :]
            q = dx * dx + dy * dy + dz * dz + ss
            inverse = lax.rsqrt(q)
            interior = (q + q + ss) * (inverse * inverse)
            value = jnp.where(tgl[rows, :] > 0.5, interior, q) * inverse
            value_high, value_low = split(value)
            k_high[rows, columns(i)] = value_high
            k_low[rows, columns(i)] = value_low
        return carry

    lax.fori_loop(0, ng, kernel_block, 0)

    def weight_block(i, carry):
        p = jnp.where(g < ng // 2, i, ng - 1 - i)

        @pl.when(p != g)
        def _():
            w_copy(p, p).wait_recv()

        w_high, w_low = split(weights[p])
        w_cat[0:systems, columns(i)] = w_high
        w_cat[systems : 2 * systems, columns(i)] = w_low
        return carry

    batch = min(ng // 2, 8)
    width = batch * own

    def product(c):
        lax.fori_loop(c * batch, (c + 1) * batch, weight_block, 0)
        cols = pl.ds(pl.multiple_of(c * width, width), width)
        both = nt_dot(w_cat[:, cols], k_high[:, cols])
        rest = nt_dot(w_cat[0:systems, cols], k_low[:, cols])
        return both[0:systems] + both[systems:] + rest

    acc[...] = product(0)
    if ng // batch > 2:

        def add_chunk(c, carry):
            acc[...] += product(c)
            return carry

        lax.fori_loop(1, ng // batch - 1, add_chunk, 0)
    total = acc[...] + product(ng // batch - 1)
    for k in range(nb):
        part[k] = total[:, k * own : (k + 1) * own]

    def img_copy(peer, slot):
        return remote(
            part.at[peer], part_in.at[slot], img_send.at[peer], img_recv.at[slot], (peer, g)
        )

    over(nb, 1, b, lambda p: img_copy(p, b).start())
    part_in[b] = part[b]
    over(nb, 1, b, lambda p: img_copy(p, p).wait_recv())
    image = part_in[0]
    for k in range(1, nb):
        image = image + part_in[k]
    image = image * (1.0 / math.sqrt(ndev * own))
    image_ref[...] = image

    image_high, image_low = split(image)
    image_cat = jnp.concatenate([image_high, image_low], axis=0)
    both = nt_dot(image_cat, sk_high[...])
    rest = nt_dot(image_high, sk_low[...])
    local = both[0:systems] + both[systems:] + rest
    for r in range(row_groups):
        for c in range(col_blocks):
            sk_part[r * col_blocks + c] = local[r * 8 : r * 8 + 8, c * 128 : c * 128 + 128]

    tile = lax.rem(me, tiles)
    base = me - tile

    def rs_copy(peer, slot):
        return remote(
            sk_part.at[lax.rem(peer, tiles)], sk_in.at[slot],
            rs_send.at[peer], rs_recv.at[slot], at(peer),
        )

    def ag_copy(peer, slot):
        return remote(
            sk_full.at[tile], sk_full.at[slot], ag_send.at[peer], ag_recv.at[slot], at(base + peer)
        )

    far_first(ndev, ng, me, lambda p: rs_copy(p, me).start())
    sk_in[me] = sk_part[tile]
    copies[5].wait()
    copies[6].wait()
    over(ndev, 1, me, lambda p: rs_copy(p, p).wait_recv())

    reach = min(ndev, 32)

    def add_tiles(i, value):
        for k in range(reach):
            value = value + sk_in[i * reach + k]
        return value

    if ndev == reach:
        summed = add_tiles(0, jnp.zeros((8, 128), F32))
    else:
        summed = lax.fori_loop(0, ndev // reach, add_tiles, jnp.zeros((8, 128), F32))
    sk_full[tile] = summed
    far_first(tiles, min(ng, tiles), tile, lambda p: ag_copy(p, tile).start())
    over(tiles, 1, tile, lambda p: ag_copy(p, p).wait_recv())

    lanes = lax.broadcasted_iota(jnp.int32, (8, 128), 1)
    for r in range(row_groups):
        rows = pl.ds(r * 8, 8)
        rest = [sk_full[r * col_blocks + c] for c in range(col_blocks)]
        coefs = []
        table = jnp.zeros((8, 128), F32)
        for j in range(vectors):
            run = rest[0] * basis[j, rows, 0:128]
            for c in range(1, col_blocks):
                run = run + rest[c] * basis[j, rows, c * 128 : c * 128 + 128]
            value = jnp.sum(run, axis=1, keepdims=True)
            coefs.append(value)
            table = jnp.where(lanes == j, value, table)
        squares = jnp.zeros((8, 128), F32)
        left = []
        for c in range(col_blocks):
            value = rest[c]
            for j in range(vectors):
                value = value - coefs[j] * basis[j, rows, c * 128 : c * 128 + 128]
            squares = squares + value * value
            left.append(value)
        mean = jnp.sum(squares, axis=1, keepdims=True) * (1.0 / (col_blocks * 128))
        norm = jnp.sqrt(mean + 1e-06)
        inverse = 1.0 / norm
        for c in range(col_blocks):
            sketch_next_ref[rows, c * 128 : c * 128 + 128] = left[c] * inverse
        vector = image_ref[rows, :]
        for j in range(vectors):
            vector = vector - coefs[j] * krylov[j, rows, :]
        next_ref[rows, :] = vector * inverse
        cmat[rows, :] = jnp.where(lanes == vectors, norm, table)
    turned = jnp.transpose(cmat[...])
    coef_ref[...] = turned[0:vectors, :]
    norms_ref[...] = turned[vectors : vectors + 1, :]

    over(nb, 1, b, lambda p: tgt_copy(p, b).wait_send())
    over(ng, 1, g, lambda p: geo_copy(p, g).wait_send())
    over(ng, 1, g, lambda p: w_copy(p, g).wait_send())
    over(nb, 1, b, lambda p: img_copy(p, b).wait_send())
    over(ndev, 1, me, lambda p: rs_copy(p, me).wait_send())
    over(tiles, 1, tile, lambda p: ag_copy(p, tile).wait_send())


def place_kernel(count, *refs):
    sems = refs[2 * count]
    outward = [pltpu.make_async_copy(refs[k], refs[count + k], sems.at[k]) for k in range(count)]
    for copy in outward:
        copy.start()
    for copy in outward:
        copy.wait()


def place(arrays):
    count = len(arrays)
    return pl.pallas_call(
        functools.partial(place_kernel, count),
        out_shape=tuple(jax.ShapeDtypeStruct(a.shape, a.dtype) for a in arrays),
        in_specs=[pl.BlockSpec(memory_space=pltpu.VMEM)] * count,
        out_specs=(pl.BlockSpec(memory_space=pltpu.HBM),) * count,
        scratch_shapes=[pltpu.SemaphoreType.DMA((count,))],
        compiler_params=pltpu.CompilerParams(vmem_limit_bytes=1024 * 1024),
    )(*arrays)


def shards(nb, ng, points, labels, shape_scale, krylov_basis, sketch, sketched_basis):
    own = points.shape[1]
    vectors, systems, _ = krylov_basis.shape
    sketch_rows = sketch.shape[0]
    ndev = nb * ng
    tiles = (systems // 8) * (sketch_rows // 128)
    assert ndev % tiles == 0
    vmem = pltpu.VMEM
    dma = pltpu.SemaphoreType.DMA
    hbm = pl.BlockSpec(memory_space=pltpu.HBM)
    out = pl.BlockSpec(memory_space=pltpu.VMEM)
    operands = [
        pltpu.with_memory_space_constraint(operand, pltpu.HBM)
        for operand in (
            points, labels.reshape(1, own), shape_scale.reshape(1, own),
            krylov_basis, sketch, sketched_basis,
        )
    ]
    results = pl.pallas_call(
        functools.partial(step_kernel, nb, ng),
        out_shape=(
            jax.ShapeDtypeStruct((systems, own), F32),
            jax.ShapeDtypeStruct((vectors, systems), F32),
            jax.ShapeDtypeStruct((systems, sketch_rows), F32),
            jax.ShapeDtypeStruct((1, systems), F32),
        ),
        in_specs=[hbm] * 6,
        out_specs=(out,) * 4,
        scratch_shapes=[
            vmem((3, own), F32), vmem((1, own), jnp.int32), vmem((1, own), F32),
            vmem(krylov_basis.shape, F32), vmem(sketch.shape, F32), vmem(sketched_basis.shape, F32),
            vmem((8, own), F32), vmem((ng, 8, own), F32), vmem((nb, 8, own), F32),
            vmem((ng, systems, own), F32),
            vmem((nb * own, own), F32), vmem((nb * own, own), F32),
            vmem((nb * own, own), F32), vmem((nb * own, own), F32),
            vmem((nb * own, ng * own), BF16), vmem((nb * own, ng * own), BF16),
            vmem((2 * systems, ng * own), BF16), vmem((systems, nb * own), F32),
            vmem((nb, systems, own), F32), vmem((nb, systems, own), F32), vmem((systems, own), F32),
            vmem(sketch.shape, BF16), vmem(sketch.shape, BF16),
            vmem((tiles, 8, 128), F32), vmem((ndev, 8, 128), F32), vmem((tiles, 8, 128), F32),
            vmem((systems, 128), F32),
            dma((7,)), dma((ng,)), dma((ng,)), dma((ng,)), dma((ng,)), dma((nb,)), dma((nb,)),
            dma((nb,)), dma((nb,)), dma((ndev,)), dma((ndev,)), dma((tiles,)), dma((tiles,)),
        ],
        compiler_params=pltpu.CompilerParams(
            collective_id=0, has_side_effects=True, vmem_limit_bytes=48 * 1024 * 1024
        ),
    )(*operands)
    next_vector, coefficients, sketch_next, norms = place(results)
    return (next_vector, coefficients, sketch_next, norms.reshape(systems))


def solution(mesh):
    placed = (
        P(None, ("blk", "grp")),
        P(("blk", "grp")),
        P(("blk", "grp")),
        P(None, None, ("blk", "grp")),
        P(None, ("blk", "grp")),
        P(),
    )
    return jax.shard_map(
        functools.partial(shards, mesh.shape["blk"], mesh.shape["grp"]),
        mesh=mesh,
        in_specs=placed,
        out_specs=(P(None, ("blk", "grp")), P(), P(), P()),
        check_vma=False,
    )
```
